32 devices in a mesh: clips: 2 (over x), seq: 16 (over z, y, core).
Axes of the slice: x: 2, y: 2, z: 4, core: 2. Of those that a mesh axis runs over, the one named last changes fastest.
Arguments:
- video_q: bfloat16 [4096, 1536], P(('clips', 'seq')), parts along dimension 0, may hold values from -200 to 200
- video_k: bfloat16 [4096, 1536], P(('clips', 'seq')), parts along dimension 0, may hold values from -7 to 7
- video_v: bfloat16 [4096, 1536], P(('clips', 'seq')), parts along dimension 0, may hold values from -6 to 6
- audio_q: bfloat16 [256, 1536], P(('clips', 'seq')), parts along dimension 0, may hold values from -200 to 200
- audio_k: bfloat16 [256, 1536], P(('clips', 'seq')), parts along dimension 0, may hold values from -6 to 6
- audio_v: bfloat16 [256, 1536], P(('clips', 'seq')), parts along dimension 0, may hold values from -6 to 6
- radius: int32 [32], P(('clips', 'seq')), parts along dimension 0, may hold values from 1 to 2
- tile_list: int32 [32, 5], P('clips'), parts along dimension 0, may hold values from -1 to 15, as said below
- tile_count: int32 [32], P('clips'), parts along dimension 0, may hold values from 1 to 5, as said below
- video_gain: float32 [1536], replicated, may hold values from 0.5 to 1.5
- audio_gain: float32 [1536], replicated, may hold values from 0.5 to 1.5
Outputs:
- video_out: bfloat16 [4096, 1536], P(('clips', 'seq')), parts along dimension 0
- audio_out: bfloat16 [256, 1536], P(('clips', 'seq')), parts along dimension 0
The draws below stay inside these ranges and needn't reach their ends.
There are 2 independent parts, one for each index of `clips`. The reference program is written for one: setup_inputs(seed, part) draws one part's arguments, and reference() takes and returns one part's arrays. A program takes and returns all parts, laid end to end along the dimension named above; an argument that names none is the same for every part. Nothing has to cross between parts.
Inputs may be any that keep to these rules, and one draw needn't show every extreme that they name: `tile_list`: row b names tile b first, then tile_count[b] - 1 distinct other tiles within 4 of b; the remaining entries are -1. `tile_count`: some block lists 5 tiles.
All inputs are finite; a program needn't handle non-finite values.
Results may differ from the reference program's by a relative error of at most 0.014.
Values may be sent and summed in bfloat16 or wider, within the bound.
A program may use at most 64 MiB of HBM per device.

```python
import jax
import jax.numpy as jnp
from jax import lax

H = 12
HD = 128
D = 1536
TOK_DEV = 128
AUD_DEV = 8
RMAX = 2
SPAN = 4
LMAX = 5
TILES = 16
NV = 2048
NA = 128


def key_field(key):
    drawn = jnp.clip(jax.random.normal(jax.random.fold_in(key, 101), (NV, D), jnp.float32), -6.0, 6.0)
    return drawn


def draw_video_k(key, part):
    return key_field(key).astype(jnp.bfloat16)


def draw_video_q(key, part):
    drawn = jnp.clip(jax.random.normal(jax.random.fold_in(key, 103), (NV, D), jnp.float32), -6.0, 6.0)
    return drawn.astype(jnp.bfloat16)


def draw_audio_q(key, part):
    drawn = jnp.clip(jax.random.normal(jax.random.fold_in(key, 106), (NA, D), jnp.float32), -6.0, 6.0)
    return drawn.astype(jnp.bfloat16)


def tile_tables(key):
    base_key = jax.random.fold_in(key, 201)
    block_counts = jax.random.randint(jax.random.fold_in(base_key, 1), (TILES,), 1, LMAX + 1)
    full_block = jax.random.randint(jax.random.fold_in(base_key, 2), (), 0, TILES)
    block_counts = jnp.where(jnp.arange(TILES) == full_block, LMAX, block_counts).astype(jnp.int32)
    candidate_offsets = jnp.concatenate([jnp.arange(-SPAN, 0), jnp.arange(1, SPAN + 1)])
    blocks = jnp.arange(TILES)[:, None]
    candidate = blocks + candidate_offsets[None, :]
    usable = (candidate >= 0) & (candidate < TILES)
    width_index = jnp.arange(2 * SPAN)[None, :]
    random_score = jax.random.randint(jax.random.fold_in(base_key, 3), (TILES, 2 * SPAN), 0, 1024) * 64 + width_index
    rank_score = jnp.where(usable, random_score, (1 << 20) + width_index)
    ordering = jnp.argsort(rank_score, axis=1, stable=True)
    picked = jnp.take_along_axis(candidate, ordering[:, :LMAX - 1], axis=1)
    tile_rows = jnp.concatenate([blocks, picked], axis=1)
    tile_rows = jnp.where(jnp.arange(LMAX)[None, :] < block_counts[:, None], tile_rows, -1)
    return (tile_rows.astype(jnp.int32), block_counts)


def draw_tile_list(key, part):
    return tile_tables(key)[0]


def draw_tile_count(key, part):
    return tile_tables(key)[1]


def place_ends(values, rng, smallest, high):
    dims = values.shape
    place = [jax.random.randint(jax.random.fold_in(rng, axis), (), 0, dims[axis]) for axis in range(len(dims))]
    values = values.at[tuple(place)].set(smallest)
    longest = dims.index(max(dims))
    place[longest] = (place[longest] + 1) % dims[longest]
    return values.at[tuple(place)].set(high)


def levels(rng, extent, split, least, high):
    loudness = 1.0
    for axis_at, shards_of in split:
        steps = jax.random.uniform(jax.random.fold_in(jax.random.fold_in(rng, 6), axis_at), (shards_of,), jnp.float32, least / len(split), high / len(split))
        loudness = loudness * jnp.repeat(jnp.exp(steps), extent[axis_at] // shards_of).reshape((-1,) + (1,) * (len(extent) - 1 - axis_at))
    return loudness


def centred(rng, extent, deviation, most, cuts=(), held_as=jnp.bfloat16):
    values = jax.random.normal(rng, extent, jnp.float32) * deviation
    if len(cuts) > 0:
        values = levels(rng, extent, cuts, -0.22, 0.18) * values
    return jnp.clip(values, min=-most, max=most).astype(held_as)


def setup_inputs(seed: int = 0, part: int = 0) -> dict:
    arg_keys = jax.random.split(jax.random.key(seed), 12)
    part_keys = jax.random.split(jax.random.fold_in(arg_keys[11], part), 12)
    video_q = draw_video_q(jax.random.fold_in(jax.random.fold_in(arg_keys[11], part), 71), part)
    video_k = draw_video_k(jax.random.fold_in(jax.random.fold_in(arg_keys[11], part), 71), part)
    video_v = centred(part_keys[2], (NV, D), 1.0, 6.0, ((0, 16),))
    audio_q = draw_audio_q(jax.random.fold_in(jax.random.fold_in(arg_keys[11], part), 71), part)
    audio_k = centred(part_keys[4], (NA, D), 1.0, 6.0, ((0, 16),))
    audio_v = centred(part_keys[5], (NA, D), 1.0, 6.0, ((0, 16),))
    radius = place_ends(jax.random.randint(part_keys[6], (TILES,), 1, RMAX + 1), jax.random.fold_in(part_keys[6], 1), 1, RMAX).astype(jnp.int32)
    tile_list = draw_tile_list(jax.random.fold_in(jax.random.fold_in(arg_keys[11], part), 71), part)
    tile_count = draw_tile_count(jax.random.fold_in(jax.random.fold_in(arg_keys[11], part), 71), part)
    video_gain = jnp.clip(1.0 + 0.1 * jax.random.normal(arg_keys[9], (D,), jnp.float32), 0.5, 1.5)
    audio_gain = jnp.clip(1.0 + 0.1 * jax.random.normal(arg_keys[10], (D,), jnp.float32), 0.5, 1.5)
    return dict(video_q=video_q, video_k=video_k, video_v=video_v, audio_q=audio_q, audio_k=audio_k, audio_v=audio_v, radius=radius, tile_list=tile_list, tile_count=tile_count, video_gain=video_gain, audio_gain=audio_gain)


negative_big = -1e+30
epsilon = 1e-06

def split_heads(matrix):
    return matrix.astype(jnp.float32).reshape(matrix.shape[0], H, HD)

def softmax_attend(queries, key_rows, value_rows, key_valid):
    scores = jnp.einsum('qhd,khd->hqk', split_heads(queries), split_heads(key_rows)) * HD ** (-0.5)
    scores = jnp.where(key_valid[None, None, :], scores, negative_big)
    row_peak = lax.optimization_barrier(jnp.max(scores, axis=-1, keepdims=True))
    weights = jnp.exp(scores - row_peak).astype(jnp.bfloat16)
    weights = lax.optimization_barrier(weights).astype(jnp.float32)
    weight_sum = lax.optimization_barrier(jnp.sum(weights, axis=-1))
    mixed = jnp.einsum('hqk,khd->hqd', weights, split_heads(value_rows)) / weight_sum[..., None]
    return jnp.transpose(mixed, (1, 0, 2)).reshape(queries.shape[0], H * HD)

def rms_scale(mixed, gain):
    mean_square = lax.optimization_barrier(jnp.mean(mixed * mixed, axis=-1, keepdims=True))
    return (mixed * lax.rsqrt(mean_square + epsilon) * gain.astype(jnp.float32)).astype(jnp.bfloat16)

def reference(video_q, video_k, video_v, audio_q, audio_k, audio_v, radius, tile_list, tile_count, video_gain, audio_gain):
    span_tiles = 2 * RMAX + 1
    key_tiles = jnp.pad(video_k.reshape(TILES, TOK_DEV, D), ((RMAX, RMAX), (0, 0), (0, 0)))
    value_tiles = jnp.pad(video_v.reshape(TILES, TOK_DEV, D), ((RMAX, RMAX), (0, 0), (0, 0)))
    query_tiles = video_q.reshape(TILES, TOK_DEV, D)
    offsets = jnp.arange(-RMAX, RMAX + 1, dtype=jnp.int32)

    def video_tile(tile_index):
        start = (tile_index, jnp.int32(0), jnp.int32(0))
        window_keys = lax.dynamic_slice(key_tiles, start, (span_tiles, TOK_DEV, D)).reshape(span_tiles * TOK_DEV, D)
        window_values = lax.dynamic_slice(value_tiles, start, (span_tiles, TOK_DEV, D)).reshape(span_tiles * TOK_DEV, D)
        neighbour = tile_index + offsets
        tile_valid = (jnp.abs(offsets) <= radius[tile_index]) & (neighbour >= 0) & (neighbour < TILES)
        key_valid = jnp.concatenate([jnp.repeat(tile_valid, TOK_DEV), jnp.ones((NA,), dtype=bool)])
        key_rows = jnp.concatenate([window_keys, audio_k], axis=0)
        value_rows = jnp.concatenate([window_values, audio_v], axis=0)
        queries = lax.dynamic_index_in_dim(query_tiles, tile_index, 0, keepdims=False)
        return softmax_attend(queries, key_rows, value_rows, key_valid)
    video_mixed = lax.map(video_tile, jnp.arange(TILES, dtype=jnp.int32))
    video_out = rms_scale(video_mixed.reshape(NV, D), video_gain)
    audio_tiles = audio_q.reshape(TILES, AUD_DEV, D)
    video_key_tiles = video_k.reshape(TILES, TOK_DEV, D)
    video_value_tiles = video_v.reshape(TILES, TOK_DEV, D)

    def audio_block(block_index):
        listed = tile_list[block_index]
        chosen = jnp.maximum(listed, 0).astype(jnp.int32)
        key_rows = video_key_tiles[chosen].reshape(LMAX * TOK_DEV, D)
        value_rows = video_value_tiles[chosen].reshape(LMAX * TOK_DEV, D)
        entry_valid = jnp.arange(LMAX, dtype=jnp.int32) < tile_count[block_index]
        key_valid = jnp.repeat(entry_valid, TOK_DEV)
        queries = lax.dynamic_index_in_dim(audio_tiles, block_index, 0, keepdims=False)
        return softmax_attend(queries, key_rows, value_rows, key_valid)
    audio_mixed = lax.map(audio_block, jnp.arange(TILES, dtype=jnp.int32))
    audio_out = rms_scale(audio_mixed.reshape(NA, D), audio_gain)
    return (video_out, audio_out)
```

```python
import functools

import jax
import jax.numpy as jnp
from jax import lax
from jax.experimental import pallas as pl
from jax.experimental.pallas import tpu as pltpu
from jax.sharding import PartitionSpec as P

HD = 128
RMAX = 2
SPAN = 4
LOG2E = 1.4426950408889634
SCALE = HD ** (-0.5) * LOG2E
NEG = -1e30
EPS = 1e-6
MESH = pl.DeviceIdType.MESH
LAG_Z = 1
LAG_C = 2


def kernel(
    n, heads, tok, aud, lmax,
    radius, tile_list, tile_count,
    vq_hbm, vk_hbm, vv_hbm, aq_hbm, ak_hbm, av_hbm, vgain, again,
    vout, aout,
    kv, audio, qown, aqown, aqin, qx, qr, part_o, part_s, back_o, back_s, attn, aattn,
    load_sem, s_dk, r_dk, s_y, r_y, s_z, r_z, s_dy, r_dy, s_dz, r_dz,
    s_aud, r_aud, s_daud, r_daud, s_q, r_q, s_bo, r_bo, s_bs, r_bs,
):
    me = lax.axis_index("seq")
    chips = n // 2
    chip = me // 2
    core = me % 2
    mate = chip * 2 + (1 - core)
    odd = chip % 2
    across_chip = chip + 1 - 2 * odd
    across = across_chip * 2 + core
    step = 2 - 4 * odd
    fwd_chip = chip + step
    has_fwd = (fwd_chip >= 0) & (fwd_chip < chips)
    src_chip = chip - step
    has_src = (src_chip >= 0) & (src_chip < chips)
    zchip = chip - 1 + 2 * odd
    fwd = jnp.clip(fwd_chip, 0, chips - 1) * 2 + core

    barrier = pltpu.get_barrier_semaphore()

    def greet(i, _):
        pl.semaphore_signal(barrier, inc=1, device_id={"seq": (me + i) % n}, device_id_type=MESH)
        return 0

    lax.fori_loop(1, n, greet, 0)

    loads = [
        pltpu.make_async_copy(aq_hbm, aqown, load_sem.at[0]),
        pltpu.make_async_copy(ak_hbm, audio.at[me, 0], load_sem.at[1]),
        pltpu.make_async_copy(av_hbm, audio.at[me, 1], load_sem.at[2]),
        pltpu.make_async_copy(vk_hbm, kv.at[0, pl.ds(0, tok)], load_sem.at[3]),
        pltpu.make_async_copy(vv_hbm, kv.at[1, pl.ds(0, tok)], load_sem.at[4]),
        pltpu.make_async_copy(vq_hbm, qown, load_sem.at[5]),
    ]
    for load in loads:
        load.start()
    @pl.when(jnp.logical_not(has_src))
    def _():
        kv[:, pl.ds(4 * tok, 2 * tok), :] = jnp.zeros((2, 2 * tok, heads * HD), kv.dtype)

    far = []
    for slot in range(4):
        far_chip = chip + (2 if slot < 2 else -2)
        exists = (far_chip >= 0) & (far_chip < chips)
        device = jnp.clip(far_chip, 0, chips - 1) * 2 + slot % 2
        there = (2 if slot < 2 else 0) + core
        far.append((slot, exists, device, there))

        @pl.when(jnp.logical_not(exists))
        def _(slot=slot):
            aqin[slot] = jnp.zeros(aqin.shape[1:], aqin.dtype)
            back_o[slot] = jnp.zeros(back_o.shape[1:], back_o.dtype)
            back_s[slot] = jnp.zeros(back_s.shape[1:], back_s.dtype)

    pl.semaphore_wait(barrier, n - 1)

    def remote(src, dst, s, r, device):
        return pltpu.make_async_remote_copy(
            src_ref=src, dst_ref=dst, send_sem=s, recv_sem=r,
            device_id={"seq": device}, device_id_type=MESH)

    def q_copy(slot, device, there):
        return remote(aqown, aqin.at[there], s_q.at[slot], r_q.at[there], device)

    def q_arrival(slot):
        return remote(aqown, aqin.at[slot], s_q.at[slot], r_q.at[slot], mate)

    loads[0].wait()
    for slot, exists, device, there in far:
        @pl.when(exists)
        def _(slot=slot, device=device, there=there):
            q_copy(slot, device, there).start()
    loads[1].wait()
    loads[2].wait()

    def aud_copy(block, device, i):
        return remote(audio.at[block], audio.at[block], s_aud.at[i], r_aud.at[block], device)

    def daud_copy(block, i):
        return remote(audio.at[block], audio.at[block], s_daud.at[i], r_daud.at[block], mate)

    def send_audio(i, _):
        aud_copy(me, (me + 2 * i) % n, i).start()
        return 0

    lax.fori_loop(1, chips, send_audio, 0)
    daud_copy(me, 0).start()
    loads[3].wait()
    loads[4].wait()

    def cols(h):
        return pl.ds(pl.multiple_of(h * HD, HD), HD)

    def kv_head(slot, h):
        return kv.at[:, pl.ds(slot * tok, tok), cols(h)]

    def y_copy(h):
        return remote(kv_head(0, h), kv_head(2, h), s_y.at[h], r_y.at[h], across)

    def z_copy(h):
        return remote(kv_head(2, h), kv_head(4, h), s_z.at[h], r_z.at[h], fwd)

    def dy_copy(h):
        return remote(kv_head(2, h), kv_head(3, h), s_dy.at[h], r_dy.at[h], mate)

    def dz_copy(h):
        return remote(kv_head(4, h), kv_head(5, h), s_dz.at[h], r_dz.at[h], mate)

    dk = remote(kv.at[:, pl.ds(0, tok)], kv.at[:, pl.ds(tok, tok)], s_dk, r_dk, mate)

    def send_y(h, _):
        y_copy(h).start()
        return 0

    lax.fori_loop(0, heads, send_y, 0)
    dk.start()

    loads[5].wait()
    wide = jnp.concatenate([aqown[...].astype(jnp.float32), jnp.zeros((aud, heads * HD), jnp.float32)], axis=0)
    qx[...] = wide.astype(jnp.bfloat16)

    for slot, exists, device, there in far:
        @pl.when(exists)
        def _(slot=slot):
            q_arrival(slot).wait_recv()
    for pair in range(2):
        both = jnp.concatenate(
            [aqin[2 * pair].astype(jnp.float32), aqin[2 * pair + 1].astype(jnp.float32)], axis=0)
        qr[pl.ds(2 * aud * pair, 2 * aud), :] = both.astype(jnp.bfloat16)
    lane = lax.broadcasted_iota(jnp.int32, (4 * aud, HD), 1)
    part_s[...] = jnp.zeros(part_s.shape, jnp.float32)

    def dot_t(a, b):
        return lax.dot_general(a, b, (((1,), (1,)), ((), ())), preferred_element_type=jnp.float32)

    def far_head(h, _):
        s = dot_t(qr[:, cols(h)], kv[0, pl.ds(0, tok), cols(h)]) * SCALE
        m = jnp.max(s, axis=1, keepdims=True)
        w = jnp.exp2(s - m).astype(jnp.bfloat16)
        total = jnp.sum(w.astype(jnp.float32), axis=1, keepdims=True)
        o = jnp.dot(w, kv[1, pl.ds(0, tok), cols(h)], preferred_element_type=jnp.float32) / total
        for slot in range(4):
            rows = slice(slot * aud, (slot + 1) * aud)
            part_o[slot, :, cols(h)] = o[rows].astype(part_o.dtype)
            st = part_s[slot]
            st = jnp.where(lane[rows] == h, m[rows], st)
            st = jnp.where(lane[rows] == h + 64, total[rows], st)
            part_s[slot] = st
        return 0

    lax.fori_loop(0, heads, far_head, 0)

    def bo_copy(slot, device, there):
        return remote(part_o.at[slot], back_o.at[there], s_bo.at[slot], r_bo.at[there], device)

    def bs_copy(slot, device, there):
        return remote(part_s.at[slot], back_s.at[there], s_bs.at[slot], r_bs.at[there], device)

    for slot, exists, device, there in far:
        @pl.when(exists)
        def _(slot=slot, device=device, there=there):
            bo_copy(slot, device, there).start()
            bs_copy(slot, device, there).start()

    def pass_audio(i, _):
        block = (me + 2 * i) % n
        aud_copy(block, mate, i).wait_recv()
        daud_copy(block, i).start()
        return 0

    lax.fori_loop(1, chips, pass_audio, 0)

    def take_audio(i, _):
        daud_copy((mate + 2 * i) % n, i).wait_recv()
        return 0

    lax.fori_loop(0, chips, take_audio, 0)

    def lay_audio(i, _):
        for j in range(2):
            pair = jnp.concatenate(
                [audio[2 * i, j].astype(jnp.float32), audio[2 * i + 1, j].astype(jnp.float32)], axis=0)
            kv[j, pl.ds(pl.multiple_of(6 * tok + 2 * aud * i, 2 * aud), 2 * aud), :] = pair.astype(jnp.bfloat16)
        return 0

    lax.fori_loop(0, chips, lay_audio, 0)

    for slot, exists, device, there in far:
        @pl.when(exists)
        def _(slot=slot):
            bo_copy(slot, mate, slot).wait_recv()
            bs_copy(slot, mate, slot).wait_recv()
    dk.wait_recv()

    near = radius[0]
    count = tile_count[me]

    def is_listed(tile):
        listed = jnp.int32(0)
        for j in range(lmax):
            listed = jnp.where((tile_list[me, j] == tile) & (j < count), 1, listed)
        return listed > 0

    tiles = [me, mate, across, across_chip * 2 + 1 - core, zchip * 2 + core, zchip * 2 + 1 - core]
    see_v, see_a = [], []
    for tile in tiles:
        inside = (tile >= 0) & (tile < n)
        see_v.append(jnp.where(inside & (jnp.abs(tile - me) <= near), 0.0, NEG).astype(jnp.float32))
        see_a.append(jnp.where(inside & is_listed(tile), 0.0, NEG).astype(jnp.float32))
    far_seen = []
    for slot in range(4):
        tile = (chip + (2 if slot < 2 else -2)) * 2 + slot % 2
        ok = (tile >= 0) & (tile < n) & is_listed(tile)
        far_seen.append(jnp.where(ok, 0.0, NEG).astype(jnp.float32))

    span = 6 * tok
    keys = span + n * aud
    lane8 = lax.broadcasted_iota(jnp.int32, (aud, HD), 1)

    def softmax_part(s, biases):
        blocks = [s[:, i * tok:(i + 1) * tok] * SCALE + biases[i] for i in range(len(biases))]
        if s.shape[1] > len(biases) * tok:
            blocks.append(s[:, len(biases) * tok:] * SCALE)
        m = functools.reduce(jnp.maximum, [jnp.max(b, axis=1, keepdims=True) for b in blocks]) if blocks[-1].shape[1] != tok else jnp.max(functools.reduce(jnp.maximum, blocks), axis=1, keepdims=True)
        w = jnp.concatenate([jnp.exp2(b - m).astype(jnp.bfloat16) for b in blocks], axis=1)
        return m, w

    def head(h):
        q = jnp.concatenate([qown[:, cols(h)], qx[:, cols(h)]], axis=0)
        s = dot_t(q, kv[0, :, cols(h)])
        _, wv = softmax_part(s[:tok], see_v)
        ma, wa = softmax_part(s[tok:, :span], see_a)
        wa = jnp.concatenate([wa, jnp.zeros((2 * aud, keys - span), jnp.bfloat16)], axis=1)
        w = jnp.concatenate([wv, wa], axis=0)
        v = kv[1, :, cols(h)]
        o = jnp.dot(w, jnp.concatenate([v, jnp.ones((keys, HD), jnp.bfloat16)], axis=1), preferred_element_type=jnp.float32)
        attn[:, cols(h)] = o[:tok, :HD] / o[:tok, HD:]
        oa = o[tok:tok + aud, :HD]
        la = o[tok:tok + aud, HD:]
        ma = ma[:aud]
        peaks, sums = [], []
        for slot in range(4):
            st = back_s[slot]
            peaks.append(jnp.max(jnp.where(lane8 == h, st, NEG), axis=1, keepdims=True) + far_seen[slot])
            sums.append(jnp.sum(jnp.where(lane8 == h + 64, st, 0.0), axis=1, keepdims=True))
        peak = functools.reduce(jnp.maximum, peaks, ma)
        shrink = jnp.exp2(ma - peak)
        oa = oa * shrink
        la = la * shrink
        for slot in range(4):
            share = jnp.exp2(peaks[slot] - peak) * sums[slot]
            oa = oa + back_o[slot, :, cols(h)].astype(jnp.float32) * share
            la = la + share
        aattn[:, cols(h)] = oa / la

    def relay(i, _):
        @pl.when(i < heads)
        def _():
            y_copy(i).wait_recv()

            @pl.when(has_fwd)
            def _():
                z_copy(i).start()
            dy_copy(i).start()

        @pl.when((i >= LAG_Z) & (i < heads + LAG_Z) & has_src)
        def _():
            z_copy(i - LAG_Z).wait_recv()
            dz_copy(i - LAG_Z).start()

        @pl.when(i >= LAG_C)
        def _():
            h = i - LAG_C
            dy_copy(h).wait_recv()

            @pl.when(has_src)
            def _():
                dz_copy(h).wait_recv()
            head(h)
        return 0

    lax.fori_loop(0, heads + LAG_C, relay, 0)

    def finish(mixed, gain):
        scale = lax.rsqrt(jnp.mean(mixed * mixed, axis=1, keepdims=True) + EPS)
        return (mixed * scale * gain).astype(jnp.bfloat16)

    vout[...] = finish(attn[...], vgain[...].reshape(1, heads * HD))
    aout[...] = finish(aattn[...], again[...].reshape(1, heads * HD))

    for slot, exists, device, there in far:
        @pl.when(exists)
        def _(slot=slot, device=device, there=there):
            q_copy(slot, device, there).wait_send()
            bo_copy(slot, device, there).wait_send()
            bs_copy(slot, device, there).wait_send()

    def audio_left(i, _):
        aud_copy(me, mate, i).wait_send()
        return 0

    lax.fori_loop(1, chips, audio_left, 0)

    def daudio_left(i, _):
        daud_copy(me, i).wait_send()
        return 0

    lax.fori_loop(0, chips, daudio_left, 0)
    dk.wait_send()

    def heads_left(h, _):
        y_copy(h).wait_send()
        dy_copy(h).wait_send()

        @pl.when(has_fwd)
        def _():
            z_copy(h).wait_send()

        @pl.when(has_src)
        def _():
            dz_copy(h).wait_send()
        return 0

    lax.fori_loop(0, heads, heads_left, 0)


def solution(mesh):
    n = mesh.shape["seq"]
    chips = n // 2

    def on_device(vq, vk, vv, aq, ak, av, radius, tile_list, tile_count, vgain, again):
        tok, width = vq.shape
        aud = aq.shape[0]
        heads = width // HD
        keys = 6 * tok + n * aud
        bf, f32 = jnp.bfloat16, jnp.float32
        dma = pltpu.SemaphoreType.DMA
        per_head = dma((heads,))
        smem = pl.BlockSpec(memory_space=pltpu.SMEM)
        anyw = pl.BlockSpec(memory_space=pl.ANY)
        vmem = pl.BlockSpec(memory_space=pltpu.VMEM)
        return pl.pallas_call(
            functools.partial(kernel, n, heads, tok, aud, tile_list.shape[1]),
            out_shape=(jax.ShapeDtypeStruct(vq.shape, bf), jax.ShapeDtypeStruct(aq.shape, bf)),
            in_specs=[smem] * 3 + [anyw] * 6 + [vmem] * 2,
            out_specs=(vmem, vmem),
            scratch_shapes=[
                pltpu.VMEM((2, keys, width), bf),
                pltpu.VMEM((n, 2, aud, width), bf),
                pltpu.VMEM((tok, width), bf),
                pltpu.VMEM((aud, width), bf),
                pltpu.VMEM((4, aud, width), bf),
                pltpu.VMEM((2 * aud, width), bf),
                pltpu.VMEM((4 * aud, width), bf),
                pltpu.VMEM((4, aud, width), bf),
                pltpu.VMEM((4, aud, HD), f32),
                pltpu.VMEM((4, aud, width), bf),
                pltpu.VMEM((4, aud, HD), f32),
                pltpu.VMEM((tok, width), f32),
                pltpu.VMEM((aud, width), f32),
                dma((6,)), dma, dma,
                *([per_head] * 8),
                dma((chips,)), dma((n,)), dma((chips,)), dma((n,)),
                *([dma((4,))] * 6),
            ],
            compiler_params=pltpu.CompilerParams(
                collective_id=0, has_side_effects=True, vmem_limit_bytes=48 * 1024 * 1024),
        )(radius, tile_list, tile_count, vq, vk, vv, aq, ak, av, vgain, again)

    rows = P(("clips", "seq"), None)
    return jax.shard_map(
        on_device,
        mesh=mesh,
        in_specs=(rows,) * 6 + (P(("clips", "seq")), P("clips", None), P("clips"), P(), P()),
        out_specs=(rows, rows),
        check_vma=False,
    )
```

```python
import functools

import jax
import jax.numpy as jnp
from jax import lax
from jax.experimental import pallas as pl
from jax.experimental.pallas import tpu as pltpu
from jax.sharding import PartitionSpec as P

HD = 128
RMAX = 2
SPAN = 4
LOG2E = 1.4426950408889634
SCALE = HD ** (-0.5) * LOG2E
NEG = -1e30
EPS = 1e-6
MESH = pl.DeviceIdType.MESH
LAG_Z = 2
LAG_C = 3
WINDOW = 4
AUDIO_PASS = 6
AUDIO_READY = 7


def kernel(
    n, heads, tok, aud, lmax,
    radius, tile_list, tile_count,
    vq_hbm, vk_hbm, vv_hbm, aq_hbm, ak_hbm, av_hbm, vgain_hbm, again_hbm,
    vout, aout,
    kv, audio, qown, aqown, aqin, qx, qr, part_o, part_s, back_o, back_s, attn, aattn, vgain, again,
    load_sem, own_sem, s_dk, r_dk, s_y, r_y, s_z, r_z, s_dy, r_dy, s_dz, r_dz,
    s_up, s_dn, s_ya, r_aud, s_daud, r_daud, s_q, r_q, s_bo, r_bo, s_bs, r_bs,
):
    me = lax.axis_index("seq")
    chips = n // 2
    chip = me // 2
    core = me % 2
    mate = chip * 2 + (1 - core)
    odd = chip % 2
    across_chip = chip + 1 - 2 * odd
    across = across_chip * 2 + core
    step = 2 - 4 * odd
    fwd_chip = chip + step
    has_fwd = (fwd_chip >= 0) & (fwd_chip < chips)
    src_chip = chip - step
    has_src = (src_chip >= 0) & (src_chip < chips)
    zchip = chip - 1 + 2 * odd
    fwd = jnp.clip(fwd_chip, 0, chips - 1) * 2 + core

    barrier = pltpu.get_barrier_semaphore()

    def greet(device):
        pl.semaphore_signal(barrier, inc=1, device_id={"seq": device}, device_id_type=MESH)

    low, high = chip >= 2, chip + 2 < chips
    greet(across)
    greet(mate)
    for exists, far_chip in ((high, chip + 2), (low, chip - 2)):
        @pl.when(exists)
        def _(far_chip=far_chip):
            greet(jnp.clip(far_chip, 0, chips - 1) * 2)
            greet(jnp.clip(far_chip, 0, chips - 1) * 2 + 1)

    loads = [
        pltpu.make_async_copy(aq_hbm, aqown, load_sem.at[0]),
        pltpu.make_async_copy(ak_hbm, audio.at[me, 0], load_sem.at[1]),
        pltpu.make_async_copy(av_hbm, audio.at[me, 1], load_sem.at[2]),
        pltpu.make_async_copy(vq_hbm, qown, load_sem.at[3]),
        pltpu.make_async_copy(vgain_hbm, vgain, load_sem.at[4]),
        pltpu.make_async_copy(again_hbm, again, load_sem.at[5]),
    ]

    def cols(h):
        return pl.ds(pl.multiple_of(h * HD, HD), HD)

    def own_head(h):
        return [
            pltpu.make_async_copy(side.at[:, cols(h)], kv.at[h, j, pl.ds(0, tok)], own_sem.at[h, j])
            for j, side in enumerate((vk_hbm, vv_hbm))
        ]

    for load in loads[:3]:
        load.start()

    def load_own(h, _):
        for load in own_head(h):
            load.start()
        return 0

    lax.fori_loop(0, heads, load_own, 0)
    for load in loads[3:]:
        load.start()
    @pl.when(jnp.logical_not(has_src))
    def _():
        def clear(h, _):
            kv[h, :, pl.ds(4 * tok, 2 * tok), :] = jnp.zeros((2, 2 * tok, HD), kv.dtype)
            return 0

        lax.fori_loop(0, heads, clear, 0)

    far = []
    for slot in range(4):
        far_chip = chip + (2 if slot < 2 else -2)
        exists = (far_chip >= 0) & (far_chip < chips)
        device = jnp.clip(far_chip, 0, chips - 1) * 2 + slot % 2
        there = (2 if slot < 2 else 0) + core
        far.append((slot, exists, device, there))

        @pl.when(jnp.logical_not(exists))
        def _(slot=slot):
            aqin[slot] = jnp.zeros(aqin.shape[1:], aqin.dtype)
            back_o[slot] = jnp.zeros(back_o.shape[1:], back_o.dtype)
            back_s[slot] = jnp.zeros(back_s.shape[1:], back_s.dtype)

    pl.semaphore_wait(barrier, 2 + 2 * high.astype(jnp.int32) + 2 * low.astype(jnp.int32))

    def remote(src, dst, s, r, device):
        return pltpu.make_async_remote_copy(
            src_ref=src, dst_ref=dst, send_sem=s, recv_sem=r,
            device_id={"seq": device}, device_id_type=MESH)

    def q_copy(slot, device, there):
        return remote(aqown, aqin.at[there], s_q.at[slot], r_q.at[there], device)

    def q_arrival(slot):
        return remote(aqown, aqin.at[slot], s_q.at[slot], r_q.at[slot], mate)

    loads[0].wait()
    for slot, exists, device, there in far:
        @pl.when(exists)
        def _(slot=slot, device=device, there=there):
            q_copy(slot, device, there).start()
    loads[1].wait()
    loads[2].wait()

    row, rows_all = chip // 2, chips // 2
    up_to = jnp.clip(chip + 2, 0, chips - 1) * 2 + core
    down_to = jnp.clip(chip - 2, 0, chips - 1) * 2 + core

    def aud_copy(sems, block, device):
        return remote(audio.at[block], audio.at[block], sems.at[block], r_aud.at[block], device)

    def daud_copy(block):
        return remote(audio.at[block], audio.at[block], s_daud.at[block], r_daud.at[block], mate)

    def spread_up(block):
        return aud_copy(s_up, block, up_to)

    def spread_down(block):
        return aud_copy(s_dn, block, down_to)

    def spread_across(block):
        return aud_copy(s_ya, block, across)

    def from_below(d, act):
        @pl.when(row - d >= 0)
        def _():
            block = jnp.maximum(me - 4 * d, 0)
            act(block)

    def from_above(d, act):
        @pl.when(row + d < rows_all)
        def _():
            block = jnp.minimum(me + 4 * d, n - 1)
            act(block)

    @pl.when(high)
    def _():
        spread_up(me).start()

    @pl.when(low)
    def _():
        spread_down(me).start()

    def column_step(d):
        def below(block):
            spread_up(block).wait_recv()

            @pl.when(high)
            def _():
                spread_up(block).start()
            spread_across(block).start()
            daud_copy(block).start()

        def above(block):
            spread_down(block).wait_recv()

            @pl.when(low)
            def _():
                spread_down(block).start()
            spread_across(block).start()
            daud_copy(block).start()

        from_below(d, below)
        from_above(d, above)

    def pass_audio(i, _):
        block = 4 * i + across % 4
        spread_across(block).wait_recv()
        daud_copy(block).start()
        return 0

    def take_audio(i, _):
        daud_copy(2 * i + 1 - core).wait_recv()
        return 0

    def kv_head(slot, h):
        return kv.at[h, :, pl.ds(slot * tok, tok)]

    def y_copy(h):
        return remote(kv_head(0, h), kv_head(2, h), s_y.at[h], r_y.at[h], across)

    def z_copy(h):
        return remote(kv_head(2, h), kv_head(4, h), s_z.at[h], r_z.at[h], fwd)

    def dy_copy(h):
        return remote(kv_head(2, h), kv_head(3, h), s_dy.at[h], r_dy.at[h], mate)

    def dz_copy(h):
        return remote(kv_head(4, h), kv_head(5, h), s_dz.at[h], r_dz.at[h], mate)

    dk = remote(kv.at[:, :, pl.ds(0, tok)], kv.at[:, :, pl.ds(tok, tok)], s_dk, r_dk, mate)

    def own_there(h, _):
        for load in own_head(h):
            load.wait()
        return 0

    for h in range(2):
        own_there(h, 0)
        y_copy(h).start()
    spread_across(me).start()
    daud_copy(me).start()
    lax.fori_loop(2, heads, own_there, 0)
    for h in range(2, WINDOW):
        y_copy(h).start()
    dk.start()

    loads[3].wait()
    wide = jnp.concatenate([aqown[...].astype(jnp.float32), jnp.zeros((aud, heads * HD), jnp.float32)], axis=0)
    qx[...] = wide.astype(jnp.bfloat16)

    def dot_t(a, b):
        return lax.dot_general(a, b, (((1,), (1,)), ((), ())), preferred_element_type=jnp.float32)

    lane = lax.broadcasted_iota(jnp.int32, (4 * aud, HD), 1)

    def far_head(h, _):
        s = dot_t(qr[:, cols(h)], kv[h, 0, pl.ds(0, tok)]) * SCALE
        m = jnp.max(s, axis=1, keepdims=True)
        w = jnp.exp2(s - m).astype(jnp.bfloat16)
        total = jnp.sum(w.astype(jnp.float32), axis=1, keepdims=True)
        o = jnp.dot(w, kv[h, 1, pl.ds(0, tok)], preferred_element_type=jnp.float32) / total
        for slot in range(4):
            rows = slice(slot * aud, (slot + 1) * aud)
            part_o[slot, :, cols(h)] = o[rows].astype(part_o.dtype)
            st = part_s[slot]
            st = jnp.where(lane[rows] == h, m[rows], st)
            st = jnp.where(lane[rows] == h + 64, total[rows], st)
            part_s[slot] = st
        return 0

    def bo_copy(slot, device, there):
        return remote(part_o.at[slot], back_o.at[there], s_bo.at[slot], r_bo.at[there], device)

    def bs_copy(slot, device, there):
        return remote(part_s.at[slot], back_s.at[there], s_bs.at[slot], r_bs.at[there], device)

    def far_part():
        for slot, exists, device, there in far:
            @pl.when(exists)
            def _(slot=slot):
                q_arrival(slot).wait_recv()
        for pair in range(2):
            both = jnp.concatenate(
                [aqin[2 * pair].astype(jnp.float32), aqin[2 * pair + 1].astype(jnp.float32)], axis=0)
            qr[pl.ds(2 * aud * pair, 2 * aud), :] = both.astype(jnp.bfloat16)
        part_s[...] = jnp.zeros(part_s.shape, jnp.float32)
        lax.fori_loop(0, heads, far_head, 0)
        for slot, exists, device, there in far:
            @pl.when(exists)
            def _(slot=slot, device=device, there=there):
                bo_copy(slot, device, there).start()
                bs_copy(slot, device, there).start()

    def lay_audio(i, _):
        for j in range(2):
            pair = jnp.concatenate(
                [audio[2 * i, j].astype(jnp.float32), audio[2 * i + 1, j].astype(jnp.float32)], axis=0)
            pair = pair.astype(jnp.bfloat16)
            for h in range(heads):
                kv[h, j, pl.ds(pl.multiple_of(6 * tok + 2 * aud * i, 2 * aud), 2 * aud), :] = pair[:, h * HD:(h + 1) * HD]
        return 0

    near = radius[0]
    count = tile_count[me]

    def is_listed(tile):
        listed = jnp.int32(0)
        for j in range(lmax):
            listed = jnp.where((tile_list[j, me] == tile) & (j < count), 1, listed)
        return listed > 0

    tiles = [me, mate, across, across_chip * 2 + 1 - core, zchip * 2 + core, zchip * 2 + 1 - core]
    see_v, see_a = [], []
    for tile in tiles:
        inside = (tile >= 0) & (tile < n)
        see_v.append(jnp.where(inside & (jnp.abs(tile - me) <= near), 0.0, NEG).astype(jnp.float32))
        see_a.append(jnp.where(inside & is_listed(tile), 0.0, NEG).astype(jnp.float32))
    far_seen = []
    for slot in range(4):
        tile = (chip + (2 if slot < 2 else -2)) * 2 + slot % 2
        ok = (tile >= 0) & (tile < n) & is_listed(tile)
        far_seen.append(jnp.where(ok, 0.0, NEG).astype(jnp.float32))

    span = 6 * tok
    keys = span + n * aud
    lane8 = lax.broadcasted_iota(jnp.int32, (aud, HD), 1)

    def softmax_part(s, biases):
        blocks = [s[:, i * tok:(i + 1) * tok] * SCALE + biases[i] for i in range(len(biases))]
        if s.shape[1] > len(biases) * tok:
            blocks.append(s[:, len(biases) * tok:] * SCALE)
        m = functools.reduce(jnp.maximum, [jnp.max(b, axis=1, keepdims=True) for b in blocks]) if blocks[-1].shape[1] != tok else jnp.max(functools.reduce(jnp.maximum, blocks), axis=1, keepdims=True)
        w = jnp.concatenate([jnp.exp2(b - m).astype(jnp.bfloat16) for b in blocks], axis=1)
        return m, w

    def head(h):
        q = jnp.concatenate([qown[:, cols(h)], qx[:, cols(h)]], axis=0)
        s = dot_t(q, kv[h, 0])
        _, wv = softmax_part(s[:tok], see_v)
        ma, wa = softmax_part(s[tok:, :span], see_a)
        wa = jnp.concatenate([wa, jnp.zeros((2 * aud, keys - span), jnp.bfloat16)], axis=1)
        w = jnp.concatenate([wv, wa], axis=0)
        v = kv[h, 1]
        o = jnp.dot(w, jnp.concatenate([v, jnp.ones((keys, HD), jnp.bfloat16)], axis=1), preferred_element_type=jnp.float32)
        attn[:, cols(h)] = o[:tok, :HD] / o[:tok, HD:]
        oa = o[tok:tok + aud, :HD]
        la = o[tok:tok + aud, HD:]
        ma = ma[:aud]
        peaks, sums = [], []
        for slot in range(4):
            st = back_s[slot]
            peaks.append(jnp.max(jnp.where(lane8 == h, st, NEG), axis=1, keepdims=True) + far_seen[slot])
            sums.append(jnp.sum(jnp.where(lane8 == h + 64, st, 0.0), axis=1, keepdims=True))
        peak = functools.reduce(jnp.maximum, peaks, ma)
        shrink = jnp.exp2(ma - peak)
        oa = oa * shrink
        la = la * shrink
        for slot in range(4):
            share = jnp.exp2(peaks[slot] - peak) * sums[slot]
            oa = oa + back_o[slot, :, cols(h)].astype(jnp.float32) * share
            la = la + share
        aattn[:, cols(h)] = oa / la

    def relay(i, _):
        @pl.when(i < heads)
        def _():
            y_copy(i).wait_recv()

            @pl.when(has_fwd)
            def _():
                z_copy(i).start()

            @pl.when(i + WINDOW < heads)
            def _():
                y_copy(i + WINDOW).start()
            dy_copy(i).start()

        @pl.when((i >= LAG_Z) & (i < heads + LAG_Z) & has_src)
        def _():
            z_copy(i - LAG_Z).wait_recv()
            dz_copy(i - LAG_Z).start()

        @pl.when(i == 0)
        def _():
            column_step(1)

        @pl.when(i == 1)
        def _():
            far_part()
            if rows_all > 2:
                column_step(2)

        @pl.when(i == 2)
        def _():
            def more(d, _):
                column_step(d)
                return 0

            lax.fori_loop(3, rows_all, more, 0)

        @pl.when(i == AUDIO_PASS)
        def _():
            lax.fori_loop(0, rows_all, pass_audio, 0)

        @pl.when(i == AUDIO_READY)
        def _():
            lax.fori_loop(0, chips, take_audio, 0)
            lax.fori_loop(0, chips, lay_audio, 0)
            for slot, exists, device, there in far:
                @pl.when(exists)
                def _(slot=slot):
                    bo_copy(slot, mate, slot).wait_recv()
                    bs_copy(slot, mate, slot).wait_recv()
            dk.wait_recv()

        def attend(h, _):
            dy_copy(h).wait_recv()

            @pl.when(has_src)
            def _():
                dz_copy(h).wait_recv()
            head(h)
            return 0

        lax.fori_loop(done(i - 1), done(i), attend, 0)
        return 0

    def done(i):
        return jnp.clip(jnp.minimum(2 * (i - AUDIO_READY + 1), i - LAG_C + 1), 0, heads)

    lax.fori_loop(0, heads + LAG_C, relay, 0)

    def finish(mixed, gain):
        scale = lax.rsqrt(jnp.mean(mixed * mixed, axis=1, keepdims=True) + EPS)
        return (mixed * scale * gain).astype(jnp.bfloat16)

    loads[4].wait()
    loads[5].wait()
    vout[...] = finish(attn[...], vgain[...].reshape(1, heads * HD))
    aout[...] = finish(aattn[...], again[...].reshape(1, heads * HD))

    for slot, exists, device, there in far:
        @pl.when(exists)
        def _(slot=slot, device=device, there=there):
            q_copy(slot, device, there).wait_send()
            bo_copy(slot, device, there).wait_send()
            bs_copy(slot, device, there).wait_send()

    @pl.when(high)
    def _():
        spread_up(me).wait_send()

    @pl.when(low)
    def _():
        spread_down(me).wait_send()
    spread_across(me).wait_send()

    def column_left(d, _):
        def below(block):
            @pl.when(high)
            def _():
                spread_up(block).wait_send()
            spread_across(block).wait_send()

        def above(block):
            @pl.when(low)
            def _():
                spread_down(block).wait_send()
            spread_across(block).wait_send()

        from_below(d, below)
        from_above(d, above)
        return 0

    lax.fori_loop(1, rows_all, column_left, 0)

    def daudio_left(i, _):
        daud_copy(2 * i + core).wait_send()
        return 0

    lax.fori_loop(0, chips, daudio_left, 0)
    dk.wait_send()

    def heads_left(h, _):
        y_copy(h).wait_send()
        dy_copy(h).wait_send()

        @pl.when(has_fwd)
        def _():
            z_copy(h).wait_send()

        @pl.when(has_src)
        def _():
            dz_copy(h).wait_send()
        return 0

    lax.fori_loop(0, heads, heads_left, 0)


def solution(mesh):
    n = mesh.shape["seq"]
    chips = n // 2

    def on_device(vq, vk, vv, aq, ak, av, radius, tile_list, tile_count, vgain, again):
        tok, width = vq.shape
        aud = aq.shape[0]
        heads = width // HD
        keys = 6 * tok + n * aud
        bf, f32 = jnp.bfloat16, jnp.float32
        dma = pltpu.SemaphoreType.DMA
        per_head = dma((heads,))
        smem = pl.BlockSpec(memory_space=pltpu.SMEM)
        hbm = pl.BlockSpec(memory_space=pltpu.HBM)
        vmem = pl.BlockSpec(memory_space=pltpu.VMEM)
        return pl.pallas_call(
            functools.partial(kernel, n, heads, tok, aud, tile_list.shape[1]),
            out_shape=(jax.ShapeDtypeStruct(vq.shape, bf), jax.ShapeDtypeStruct(aq.shape, bf)),
            in_specs=[smem] * 3 + [hbm] * 8,
            out_specs=(vmem, vmem),
            scratch_shapes=[
                pltpu.VMEM((heads, 2, keys, HD), bf),
                pltpu.VMEM((n, 2, aud, width), bf),
                pltpu.VMEM((tok, width), bf),
                pltpu.VMEM((aud, width), bf),
                pltpu.VMEM((4, aud, width), bf),
                pltpu.VMEM((2 * aud, width), bf),
                pltpu.VMEM((4 * aud, width), bf),
                pltpu.VMEM((4, aud, width), bf),
                pltpu.VMEM((4, aud, HD), f32),
                pltpu.VMEM((4, aud, width), bf),
                pltpu.VMEM((4, aud, HD), f32),
                pltpu.VMEM((tok, width), f32),
                pltpu.VMEM((aud, width), f32),
                pltpu.VMEM((width,), f32),
                pltpu.VMEM((width,), f32),
                dma((6,)), dma((heads, 2)), dma, dma,
                *([per_head] * 8),
                *([dma((n,))] * 6),
                *([dma((4,))] * 6),
            ],
            compiler_params=pltpu.CompilerParams(
                collective_id=0, has_side_effects=True),
        )(radius, tile_list.T, tile_count, vq, vk, vv, aq, ak, av, vgain, again)

    rows = P(("clips", "seq"), None)
    return jax.shard_map(
        on_device,
        mesh=mesh,
        in_specs=(rows,) * 6 + (P(("clips", "seq")), P("clips", None), P("clips"), P(), P()),
        out_specs=(rows, rows),
        check_vma=False,
    )
```
